32 devices in a mesh: wide: 16 (over z, y, x), narrow: 2 (over core).
Axes of the slice: x: 2, y: 2, z: 4, core: 2. Of those that a mesh axis runs over, the one named last changes fastest.
Arguments:
- contributions: float32 [2, 3, 8192, 128], P('narrow', None, 'wide'), may hold values from -6 to 6
- send_map: int32 [16, 800], P('wide'), may hold values from -1 to 511, as said below
- arrival_map: int32 [16, 800], P('wide'), may hold values from -1 to 255, as said below
- dual_diagonal: float32 [4096, 128], P('wide'), may hold values from 0.5 to 2
- mortar: bfloat16 [4096, 128, 128], P('wide'), may hold values from -0.5 to 0.5
- master_inverse: bfloat16 [4096, 128, 128], P('wide'), may hold values from -0.5 to 0.5
Outputs:
- corrections: float32 [2, 3, 8192, 128], P('narrow', None, 'wide')
The draws below stay inside these ranges and needn't reach their ends.
Inputs may be any that keep to these rules, and one draw needn't show every extreme that they name: `send_map`: each row 0 to 511 of a partition stands in exactly one of its slots. Some stripe has all 50 of its slots used by every partition. arrival_map[d, o * 50 + c] is -1 exactly where send_map[o, d * 50 + c] is -1.
All inputs are finite; a program needn't handle non-finite values.
Results may differ from the reference program's by a relative error of at most 0.0041.
Values sent between devices are 32-bit elements; how exact they have to be, the bound alone decides.
No kernel may reach another device: no remote copies, remote signals or barrier semaphores. Data moves between devices by JAX's collectives and lax.ppermute only.
A program may use at most 64 MiB of HBM per device.

```python
import math
import jax
import jax.numpy as jnp
from jax import lax

NODES = 128
COMP = 3
BLK_DEV = 256
BLOCKS = 4096
ROWS_OWN = 512
ROWS = 8192
CAP = 50
SLOTS = 800
N_WIDE = 16


def shared_maps(key):
    base = jax.random.fold_in(key, 7)
    key_hot, key_bias, key_jitter, key_tie, key_rows, key_block = jax.random.split(base, 6)
    hot_stripe = jax.random.randint(key_hot, (), 0, N_WIDE)
    stripe_bias = jax.random.randint(key_bias, (N_WIDE,), 0, 4)
    stripe_bias = stripe_bias * stripe_bias
    stripe_ids = jnp.arange(SLOTS, dtype=jnp.int32) // CAP
    random_perturbation = jax.random.randint(key_jitter, (N_WIDE, SLOTS), 0, 16)
    scores = jnp.where(stripe_ids[None, :] == hot_stripe, 1000, stripe_bias[stripe_ids][None, :] + random_perturbation)
    raw_ties = jax.random.randint(key_tie, (N_WIDE, SLOTS), 0, 1 << 30)
    tie_rank = jnp.argsort(jnp.argsort(raw_ties, axis=1), axis=1)
    priority_order = jnp.argsort(-(scores * SLOTS + tie_rank), axis=1)
    chosen = priority_order[:, :ROWS_OWN]
    row_order = jnp.argsort(jax.random.randint(key_rows, (N_WIDE, ROWS_OWN), 0, 1 << 30), axis=1).astype(jnp.int32)
    owners = jnp.arange(N_WIDE, dtype=jnp.int32)[:, None]
    send_map = jnp.full((N_WIDE, SLOTS), -1, jnp.int32).at[owners, chosen].set(row_order)
    by_stripe = jnp.transpose(send_map.reshape(N_WIDE, N_WIDE, CAP), (1, 0, 2)).reshape(N_WIDE, SLOTS)
    local_ids = jax.random.randint(key_block, (N_WIDE, SLOTS), 0, BLK_DEV)
    arrival_map = jnp.where(by_stripe >= 0, local_ids, -1).astype(jnp.int32)
    return (send_map, arrival_map)


def draw_send_map(key, part):
    return shared_maps(key)[0]


def draw_arrival_map(key, part):
    return shared_maps(key)[1]


def steps_of(key, shape, cuts, least, largest):
    def one(axis_at, shards_of):
        steps = jax.random.uniform(jax.random.fold_in(jax.random.fold_in(key, 6), axis_at), (shards_of,), jnp.float32, least / len(cuts), largest / len(cuts))
        return jnp.repeat(jnp.exp(steps), shape[axis_at] // shards_of).reshape((-1,) + (1,) * (len(shape) - axis_at - 1))

    level = one(*cuts[0])
    for cut in cuts[1:]:
        level = level * one(*cut)
    return level


def bell_draw(rng, shape, scale, most, cuts=(), kind=jnp.bfloat16):
    drawn = scale * jax.random.normal(rng, shape, jnp.float32)
    if cuts:
        drawn = drawn * steps_of(rng, shape, cuts, -0.22, 0.18)
    return jnp.clip(drawn, -most, most).astype(kind)


def setup_inputs(seed: int = 0) -> dict:
    seeds = jax.random.split(jax.random.key(seed), 7)
    return {
        "contributions": bell_draw(seeds[0], (2, COMP, ROWS, NODES), 1.0, 6.0, ((0, 2), (2, 16)), jnp.float32),
        "send_map": draw_send_map(jax.random.fold_in(seeds[6], 71), 0),
        "arrival_map": draw_arrival_map(jax.random.fold_in(seeds[6], 71), 0),
        "dual_diagonal": jnp.clip(jnp.exp(math.log(2.0) - 1.3862944 * jax.random.uniform(seeds[3], (BLOCKS, NODES), jnp.float32) ** steps_of(seeds[3], (BLOCKS, NODES), ((0, 16),), -0.2, 0.2)), 0.5, 2.0),
        "mortar": bell_draw(seeds[4], (BLOCKS, NODES, NODES), NODES ** -0.5, 0.5, ((0, 16),)),
        "master_inverse": bell_draw(seeds[5], (BLOCKS, NODES, NODES), NODES ** -0.5, 0.5, ((0, 16),)),
    }


def stripe_solve(pieces):
    summed, diagonal, mortar_part, inverse_part = pieces
    mortar_wide = mortar_part.astype(jnp.float32)
    inverse_wide = inverse_part.astype(jnp.float32)
    multiplier = summed[0] / diagonal[None]
    multiplier_low = lax.optimization_barrier(multiplier.astype(jnp.bfloat16)).astype(jnp.float32)
    pushed = jnp.einsum('bij,cbi->cbj', mortar_wide, multiplier_low, precision=lax.Precision.HIGHEST)
    condensed = summed[1] + pushed
    condensed_low = lax.optimization_barrier(condensed.astype(jnp.bfloat16)).astype(jnp.float32)
    master_fix = jnp.einsum('bkj,cbj->cbk', inverse_wide, condensed_low, precision=lax.Precision.HIGHEST)
    master_low = lax.optimization_barrier(master_fix.astype(jnp.bfloat16)).astype(jnp.float32)
    slave_fix = jnp.einsum('bij,cbj->cbi', mortar_wide, master_low, precision=lax.Precision.HIGHEST) / diagonal[None]
    return jnp.stack([slave_fix, master_fix])


def reference(contributions, send_map, arrival_map, dual_diagonal, mortar, master_inverse):
    owners = jnp.arange(N_WIDE, dtype=jnp.int32)[:, None]
    slot_ids = jnp.arange(SLOTS, dtype=jnp.int32)[None, :]
    stripes = slot_ids // CAP
    local_block = arrival_map[stripes, owners * CAP + slot_ids % CAP]
    is_live = send_map >= 0
    targets = jnp.where(is_live, owners * ROWS_OWN + send_map, ROWS).astype(jnp.int32)
    block_ids = (stripes * BLK_DEV + local_block).astype(jnp.int32)
    row_block = jnp.zeros((ROWS + 1,), jnp.int32).at[targets.reshape(-1)].set(block_ids.reshape(-1))[:ROWS]
    summed = jnp.zeros((2, COMP, BLOCKS, NODES), jnp.float32).at[:, :, row_block, :].add(contributions)
    by_stripe = jnp.transpose(summed.reshape(2, COMP, N_WIDE, BLK_DEV, NODES), (2, 0, 1, 3, 4))
    diag_parts = dual_diagonal.reshape(N_WIDE, BLK_DEV, NODES)
    mortar_parts = mortar.reshape(N_WIDE, BLK_DEV, NODES, NODES)
    inverse_parts = master_inverse.reshape(N_WIDE, BLK_DEV, NODES, NODES)
    fixes = lax.map(stripe_solve, (by_stripe, diag_parts, mortar_parts, inverse_parts))
    fixes = jnp.transpose(fixes, (1, 2, 0, 3, 4)).reshape(2, COMP, BLOCKS, NODES)
    return fixes[:, :, row_block, :]
```

```python
import functools

import jax
import jax.numpy as jnp
from jax import lax
from jax.experimental import pallas as pl
from jax.experimental.pallas import tpu as pltpu
from jax.sharding import PartitionSpec as P


VMEM = pltpu.VMEM
SMEM = pltpu.SMEM


def distance_plan(wide):
    half, quarter = wide // 2, wide // 4
    upper = list(range(half + quarter, wide))
    lower = list(range(half + 1, half + quarter))
    pairs = list(zip(upper, lower))
    pairs.append((upper[-1], quarter))
    near = [d for d in range(1, half) if d != quarter]
    pairs += list(zip(near[0::2], near[1::2]))
    return half, pairs


def hop_both(value, wide, distance):
    return lax.ppermute(value, "wide", [(i, i ^ distance) for i in range(wide)])


def hop_split(value, wide, pair):
    links = [(2 * i + core, 2 * (i ^ pair[core]) + core) for i in range(wide) for core in (0, 1)]
    return lax.ppermute(value, ("wide", "narrow"), links)


def swap_cores(value):
    return lax.ppermute(value, "narrow", [(0, 1), (1, 0)])


def copy_rows(source, target, index_of, count, offset, comps, nodes):
    for slot in range(count):
        row = index_of(slot)
        for c in range(comps):
            target[offset + slot : offset + slot + 1, c * nodes : (c + 1) * nodes] = source[
                c, pl.ds(row, 1), :
            ]


def gather_near(cap, half, place, send, own, far_out, home_out):
    comps, nodes = own.shape[0], own.shape[2]
    for out, distance in ((far_out, half), (home_out, 0)):
        base = (place[0] ^ distance) * cap
        copy_rows(own, out, lambda s: jnp.maximum(send[base + s], 0), cap, 0, comps, nodes)


def gather_pairs(cap, pairs, place, send, own, other, *outs):
    comps, nodes = own.shape[0], own.shape[2]
    for (first, second), out in zip(pairs, outs):
        base = (place[0] ^ jnp.where(place[1] == 0, first, second)) * cap
        index_of = lambda s: jnp.maximum(send[base + s], 0)
        copy_rows(own, out, index_of, cap, 0, comps, nodes)
        copy_rows(other, out, index_of, cap, cap, comps, nodes)


def add_rows(cap, half, pairs, place, spots, *refs):
    doubles, far, home, keep, give = refs[: len(pairs)], *refs[len(pairs) :]
    spot_count = keep.shape[0] + give.shape[0]
    total = None

    def add(total, rows, ids):
        count = rows.shape[0]
        hot = lax.broadcasted_iota(jnp.int32, (spot_count, count), 0) == ids
        hot = hot.astype(jnp.float32).astype(jnp.bfloat16)
        high = rows.astype(jnp.bfloat16)
        low = (rows - high.astype(jnp.float32)).astype(jnp.bfloat16)
        for part in (high, low):
            piece = jnp.dot(hot, part, preferred_element_type=jnp.float32)
            total = piece if total is None else total + piece
        return total

    for (first, second), ref in zip(pairs, doubles):
        source = place[0] ^ jnp.where(place[1] == 0, first, second)
        total = add(total, ref[...], spots[pl.ds(source, 1), :])
    for ref, distance in ((far, half), (home, 0)):
        total = add(total, ref[...], spots[pl.ds(place[0] ^ distance, 1), :cap])
    keep[...] = total[: keep.shape[0]]
    give[...] = total[keep.shape[0] :]


def solve(group, comps, place, keep, got, diagonal, mortar, inverse, out):
    nodes = diagonal.shape[1]
    blocks = diagonal.shape[0]
    row = lax.broadcasted_iota(jnp.int32, (comps * group, nodes), 0) % group

    def stage(stacked, matrix, contract):
        picked = None
        for g in range(group):
            full = lax.dot_general(
                stacked, matrix(g), (((1,), (contract,)), ((), ())), preferred_element_type=jnp.float32
            )
            picked = full if picked is None else jnp.where(row == g, full, picked)
        return picked

    def stack(value):
        return jnp.concatenate([value[:, c * nodes : (c + 1) * nodes] for c in range(comps)], axis=0)

    for start in range(0, blocks, group):
        here = pl.ds(start, group)
        scale = jnp.concatenate([diagonal[here, :]] * comps, axis=0)
        slave = stack(keep[0, here, :] + got[0, here, :])
        master = stack(keep[1, here, :] + got[1, here, :])
        multiplier = (slave / scale).astype(jnp.bfloat16)
        condensed = master + stage(multiplier, lambda g: mortar[start + g], 0)
        fix = stage(condensed.astype(jnp.bfloat16), lambda g: inverse[start + g], 1)
        back = stage(fix.astype(jnp.bfloat16), lambda g: mortar[start + g], 1) / scale
        for c in range(comps):
            lanes = slice(c * nodes, (c + 1) * nodes)
            out[0, here, lanes] = back[c * group : (c + 1) * group]
            out[1, here, lanes] = fix[c * group : (c + 1) * group]


def spread_rows(cap, half, pairs, place, spots, keep, got, *refs):
    outs, far, home, table = refs[: len(pairs)], *refs[len(pairs) :]
    side = keep.shape[0]
    table[:side] = keep[...]
    table[side:] = got[...]

    def copy(out, source, count):
        for s in range(count):
            spot = jnp.maximum(spots[source, s], 0)
            out[s : s + 1, :] = table[pl.ds(spot, 1), :]

    for (first, second), out in zip(pairs, outs):
        copy(out, place[0] ^ jnp.where(place[1] == 0, first, second), 2 * cap)
    copy(far, place[0] ^ half, cap)
    copy(home, place[0], cap)


def split_other(cap, pairs, *refs):
    doubles, out = refs[: len(pairs)], refs[len(pairs)]
    for k, ref in enumerate(doubles):
        out[k] = ref[cap:, :]


def place_rows(cap, half, pairs, place, send, swapped, *refs):
    doubles, far, home, out = refs[: len(pairs)], *refs[len(pairs) :]
    comps, _, nodes = out.shape

    def put(source, base, read):
        for s in range(cap):
            row = send[base + s]

            @pl.when(row >= 0)
            def _():
                for c in range(comps):
                    out[c, pl.ds(row, 1), :] = read(source, s, slice(c * nodes, (c + 1) * nodes))

    plain = lambda ref, s, lanes: ref[s : s + 1, lanes]
    for k, ((first, second), ref) in enumerate(zip(pairs, doubles)):
        mine = place[0] ^ jnp.where(place[1] == 0, first, second)
        theirs = place[0] ^ jnp.where(place[1] == 0, second, first)
        put(ref, mine * cap, plain)
        put(swapped, theirs * cap, lambda ref, s, lanes: ref[k, s : s + 1, lanes])
    put(far, (place[0] ^ half) * cap, plain)
    put(home, place[0] * cap, plain)


def call(body, outs, args, spaces, scratch=()):
    return pl.pallas_call(
        body,
        out_shape=outs,
        in_specs=[pl.BlockSpec(memory_space=s) for s in spaces],
        out_specs=jax.tree.map(lambda _: pl.BlockSpec(memory_space=VMEM), outs),
        scratch_shapes=scratch,
    )(*args)


def shards(wide, contributions, send_map, arrival_map, dual_diagonal, mortar, master_inverse):
    half, pairs = distance_plan(wide)
    comps, rows, nodes = contributions.shape[1:]
    blocks = dual_diagonal.shape[0]
    cap = send_map.shape[1] // wide
    part = blocks // 2
    core = lax.axis_index("narrow")
    place = jnp.stack([lax.axis_index("wide"), core]).astype(jnp.int32)
    f32 = lambda *shape: jax.ShapeDtypeStruct(shape, jnp.float32)
    single, double = f32(cap, comps * nodes), f32(2 * cap, comps * nodes)
    count = len(pairs)

    own = contributions[0]
    send = send_map[0]
    other = swap_cores(own)

    block = arrival_map[0].reshape(wide, cap)
    low = block % part + jnp.where(block // part == core, 0, 2 * part)
    spot = lambda side: jnp.where(block < 0, -1, low + side * part)
    spots = jnp.concatenate([spot(core), spot(1 - core)], axis=1)

    far_row, home_row = call(
        functools.partial(gather_near, cap, half),
        [single, single],
        (place, send, own),
        (SMEM, SMEM, VMEM),
    )
    far_row = hop_both(far_row, wide, half)
    sent = call(
        functools.partial(gather_pairs, cap, pairs),
        [double] * count,
        (place, send, own, other),
        (SMEM, SMEM, VMEM, VMEM),
    )
    came = []
    for k, pair in enumerate(pairs):
        came.append(hop_split(sent[k], wide, pair))

    keep, give = call(
        functools.partial(add_rows, cap, half, pairs),
        [f32(2 * part, comps * nodes)] * 2,
        (place, spots, *came, far_row, home_row),
        (SMEM, VMEM) + (VMEM,) * (count + 2),
    )
    got = swap_cores(give)

    steps = 4
    step = part // steps
    table = (2, part, comps * nodes)
    offset = lambda i, place: (place[1] * steps + i, 0, 0)
    fixes = pl.pallas_call(
        functools.partial(solve, 8, comps),
        out_shape=f32(*table),
        grid_spec=pltpu.PrefetchScalarGridSpec(
            num_scalar_prefetch=1,
            grid=(steps,),
            in_specs=[
                pl.BlockSpec((2, step, comps * nodes), lambda i, place: (0, i, 0)),
                pl.BlockSpec((2, step, comps * nodes), lambda i, place: (0, i, 0)),
                pl.BlockSpec((step, nodes), lambda i, place: (place[1] * steps + i, 0)),
                pl.BlockSpec((step, nodes, nodes), offset),
                pl.BlockSpec((step, nodes, nodes), offset),
            ],
            out_specs=pl.BlockSpec((2, step, comps * nodes), lambda i, place: (0, i, 0)),
        ),
        name="solve",
    )(place, keep.reshape(table), got.reshape(table), dual_diagonal, mortar, master_inverse)
    fixes = fixes.reshape(2 * part, comps * nodes)
    got_fixes = swap_cores(fixes)

    *sent, far_row, home_row = call(
        functools.partial(spread_rows, cap, half, pairs),
        [double] * count + [single, single],
        (place, spots, fixes, got_fixes),
        (SMEM, SMEM, VMEM, VMEM),
        scratch=[VMEM((4 * part, comps * nodes), jnp.float32)],
    )
    came = []
    for k, pair in enumerate(pairs):
        came.append(hop_split(sent[k], wide, pair))
    far_row = hop_both(far_row, wide, half)

    theirs = call(
        functools.partial(split_other, cap, pairs),
        f32(count, cap, comps * nodes),
        came,
        (VMEM,) * count,
    )
    swapped = swap_cores(theirs)
    placed = call(
        functools.partial(place_rows, cap, half, pairs),
        f32(comps, rows, nodes),
        (place, send, swapped, *came, far_row, home_row),
        (SMEM, SMEM) + (VMEM,) * (count + 3),
    )
    return placed[None]


def solution(mesh):
    wide = mesh.shape["wide"]
    _, _ = distance_plan(wide)

    def step(*args):
        return shards(wide, *args)

    placed = (
        P("narrow", None, "wide", None),
        P("wide", None),
        P("wide", None),
        P("wide", None),
        P("wide", None, None),
        P("wide", None, None),
    )
    return jax.shard_map(
        step,
        mesh=mesh,
        in_specs=placed,
        out_specs=P("narrow", None, "wide", None),
        check_vma=False,
    )
```
